16 devices in a mesh: dp: 2 (over y, z), sp: 8 (over x, core).
Axes of the slice: x: 4, y: 2, z: 1, core: 2. Of those that a mesh axis runs over, the one named last changes fastest.
The devices are a block of a 4x4x8 slice.
Arguments:
- x: bfloat16 [8192, 4096], P(('dp', 'sp')), parts along dimension 0
- gain: bfloat16 [4096], replicated
- wq: bfloat16 [4096, 4096], P('sp')
- wk: bfloat16 [4096, 512], P('sp')
- wv: bfloat16 [4096, 512], P('sp')
- wo: bfloat16 [4096, 4096], P('sp')
Outputs:
- output: bfloat16 [8192, 4096], P(('dp', 'sp')), parts along dimension 0
There are 2 independent parts. The reference program is written for one: setup_inputs(seed, part) draws one part's arguments, and reference() takes and returns one part's arrays. A program takes and returns all parts, laid end to end along the dimension named above; an argument that names none is the same for every part.
All inputs are finite; a program needn't handle non-finite values.
Results may differ from the reference program's by a relative error of at most 0.012.
Values are sent between devices in bfloat16 or wider.
A program may use at most 768 MiB of HBM per device.

```python
import jax
import jax.numpy as jnp
from jax import lax

ROWS = 4096
D = 4096
HEADS = 32
KV_HEADS = 4
HEAD = 128
THETA = 10000


def setup_inputs(seed: int = 0, part: int = 0) -> dict:
    kx, kn, kq, kk, kv, ko = jax.random.split(jax.random.key(seed), 6)

    def weights(key, rows, columns):
        return jax.random.normal(key, (rows, columns), jnp.float32) * rows**-0.5

    drawn = {
        "x": jax.random.normal(jax.random.fold_in(kx, part), (ROWS, D), jnp.float32),
        "gain": 1 + 0.1 * jax.random.normal(kn, (D,), jnp.float32),
        "wq": 2 * weights(kq, D, HEADS * HEAD),
        "wk": 2 * weights(kk, D, KV_HEADS * HEAD),
        "wv": 4 * weights(kv, D, KV_HEADS * HEAD),
        "wo": weights(ko, HEADS * HEAD, D),
    }
    return {k: v.astype(jnp.bfloat16) for k, v in drawn.items()}


def normed(x, gain):
    wide = x.astype(jnp.float32)
    scale = lax.rsqrt(jnp.mean(wide * wide, -1, keepdims=True) + 1e-6)
    return (wide * scale * gain.astype(jnp.float32)).astype(jnp.bfloat16)


def turned(t, place, theta):
    half = t.shape[-1] // 2
    angle = place.astype(jnp.float32)[:, None] * theta ** (-jnp.arange(half, dtype=jnp.float32) / half)
    cos, sin = jnp.cos(angle)[:, None], jnp.sin(angle)[:, None]
    a, b = t[..., :half].astype(jnp.float32), t[..., half:].astype(jnp.float32)
    return jnp.concatenate([a * cos - b * sin, b * cos + a * sin], -1).astype(jnp.bfloat16)


def matmul(a, w):
    return jnp.dot(a, w, preferred_element_type=jnp.float32).astype(jnp.bfloat16)


def einsum(form, a, b):
    return jnp.einsum(form, a.astype(jnp.float32), b.astype(jnp.float32))


def attention(q, k, v):
    scores = einsum("tgsd,ugd->gstu", q, k) * q.shape[-1] ** -0.5
    token = jnp.arange(q.shape[0])
    scores = jnp.where(token[:, None] >= token, scores, -jnp.inf)
    weights = jax.nn.softmax(scores, -1).astype(jnp.bfloat16)
    return einsum("gstu,ugd->tgsd", weights, v).astype(jnp.bfloat16)


def reference(x, gain, wq, wk, wv, wo):
    a, place = normed(x, gain), jnp.arange(ROWS)
    q = turned(matmul(a, wq).reshape(ROWS, HEADS, HEAD), place, THETA).reshape(ROWS, KV_HEADS, -1, HEAD)
    k = turned(matmul(a, wk).reshape(ROWS, KV_HEADS, HEAD), place, THETA)
    v = matmul(a, wv).reshape(ROWS, KV_HEADS, HEAD)
    seen = attention(q, k, v).reshape(ROWS, HEADS * HEAD)
    return (x.astype(jnp.float32) + jnp.dot(seen, wo, preferred_element_type=jnp.float32)).astype(jnp.bfloat16)
```

```python
import functools

import jax
import jax.numpy as jnp
from jax import lax
from jax.experimental import pallas as pl
from jax.experimental.pallas import tpu as pltpu
from jax.sharding import PartitionSpec as P

HEAD = 128
THETA = 10000
NEG = -1e30
HIDDEN = 2 * NEG
LOG2E = 1.4426950408889634
VMEM = 63 * 2**20
MESH = pl.DeviceIdType.MESH
B = 512
SHARED = {"w": 1, "q": 3, "o": 2}
KV = "kv"

BEFORE = [("own", "w", 0), ("own", "q", 0), ("own", "w", 1), ("norm",),
          ("near", "w", 0), ("far", "w", 0), ("own", "q", 1), ("near", "q", 0), ("near", "w", 1), ("far", "q", 0), ("far", "w", 1),
          ("make_kv",), ("own", KV, 0), ("own", "q", 2), ("own", "q", 7), ("near", "q", 1), ("load", "q", 0), ("near", KV, 0), ("far", "q", 1), ("far", KV, 0),
          ("have", KV, 0)]
ATTEND = [0, 7, 1, 2, 6, 3, 4, 5]
DURING = [
    [("own", "q", 3), ("near", "q", 7), ("far", "q", 7)],
    [("near", "q", 2), ("own", "q", 4), ("own", "q", 6)],
    [("far", "q", 2), ("near", "q", 3), ("near", "q", 6), ("own", "o", 0)],
    [("far", "q", 3), ("far", "q", 6), ("near", "q", 4), ("own", "o", 1)],
    [("far", "q", 4), ("near", "o", 0), ("own", "o", 2), ("own", "q", 5)],
    [("far", "o", 0), ("near", "q", 5), ("near", "o", 1), ("own", "o", 3)],
    [("far", "q", 5), ("far", "o", 1), ("near", "o", 2), ("own", "o", 4)],
    [("far", "o", 2), ("near", "o", 3), ("own", "o", 5), ("own", "o", 7), ("own", "o", 6)],
]
PROJECT = [0, 1, 7, 2, 3, 6, 4, 5]
AFTER = [
    [("far", "o", 3), ("near", "o", 7)],
    [("far", "o", 7), ("near", "o", 4)],
    [],
    [("far", "o", 4), ("near", "o", 6)],
    [("far", "o", 6), ("near", "o", 5)],
    [],
    [("far", "o", 5)],
    [],
]


def _dot(a, b, ca, cb):
    return lax.dot_general(a, b, (((ca,), (cb,)), ((), ())), preferred_element_type=jnp.float32)


def _kernel(n, paired, x_hbm, gain_ref, wq, wk, wv, wo, cos_ref, sin_ref, y_hbm, got,
            x_s, a_s, seen_s, k_s, v_s, w_s, q_s, acc_s, top_s, mix_s, y_s,
            near_sem, core_sem, send_sem, load_sem, x_sem, y_sem):
    tokens, width = x_s.shape
    pieces = {"w": 2, "q": wq.shape[1] // B, "o": wo.shape[1] // B}
    base = {"w": 0, "q": 2, "o": 2 + pieces["q"]}
    at_k = 2 + pieces["q"] + pieces["o"]
    per = B // HEAD
    group = width // HEAD // (wk.shape[1] // HEAD)

    me = lax.axis_index("sp")
    dp = lax.axis_index("dp")
    side = lax.rem(me, 2)
    odd = lax.rem(dp, 2) if paired else 0
    right, left, opp = lax.rem(me + 2, n), lax.rem(me + n - 2, n), lax.rem(me + n // 2, n)
    core = me + 1 - 2 * side
    from_near = (left, right, opp)
    from_core = (core, lax.rem(core + n - 2, n), lax.rem(core + 2, n), lax.rem(core + n // 2, n))
    to_right, to_left, to_core = {"sp": right}, {"sp": left}, {"sp": core}
    to_peer = {"dp": dp + 1 - 2 * odd}
    onward = lax.select(side == 0, right, left)
    carried = lax.select(side == 0, left, right)

    def piece(kind, j):
        return j + odd * (pieces[kind] - 1 - 2 * j)

    def index(kind, j):
        return base[kind] + piece(kind, j)

    def along_x(kind, j):
        return not paired or j < pieces[kind] - SHARED[kind]

    def exported(kind, j):
        return paired and j < SHARED[kind]

    def own_block(kind, j, act):
        if kind == "w":
            which = piece(kind, j)
            pl.when(which == 0)(lambda: act(wk))
            pl.when(which == 1)(lambda: act(wv))
        else:
            ref = wq if kind == "q" else wo
            act(ref.at[:, pl.ds(pl.multiple_of(piece(kind, j) * B, B), B)])

    def send(src, dst, send_at, recv, to):
        pltpu.make_async_remote_copy(src_ref=src, dst_ref=dst, send_sem=send_sem.at[send_at], recv_sem=recv, device_id=to,
                                     device_id_type=MESH).start()

    def arrived(ref, sem):
        pltpu.make_async_copy(ref, ref, sem).wait()

    def parts(kind, j):
        if kind == KV:
            return [(at_k, lambda s: k_s.at[s]), (at_k + 1, lambda s: v_s.at[s])]
        i = index(kind, j)
        return [(i, lambda s: got.at[i, s])]

    def own(kind, j):
        def act(src, i, block):
            if kind == KV or along_x(kind, j):
                send(src, block(me), i, near_sem.at[i, 0], to_right)
                send(src, block(me), i, near_sem.at[i, 1], to_left)
            send(src, block(me), i, core_sem.at[i, 0], to_core)

        for i, block in parts(kind, j):
            if kind == KV:
                act(block(me), i, block)
            else:
                own_block(kind, j, lambda src: act(src, i, block))

    def near(kind, j):
        for i, block in parts(kind, j):
            for slot in (0, 1):
                s = from_near[slot]
                arrived(block(s), near_sem.at[i, slot])
                if kind != KV and exported(kind, j):
                    send(block(s), block(s), i, near_sem.at[i, slot], to_peer)
            if kind == KV or along_x(kind, j):
                send(block(carried), block(carried), i, near_sem.at[i, 2], {"sp": onward})
            for slot in (0, 1):
                s = from_near[slot]
                send(block(s), block(s), i, core_sem.at[i, 1 + slot], to_core)

    def far(kind, j):
        for i, block in parts(kind, j):
            arrived(block(opp), near_sem.at[i, 2])
            if kind != KV and exported(kind, j):
                send(block(opp), block(opp), i, near_sem.at[i, 2], to_peer)
            send(block(opp), block(opp), i, core_sem.at[i, 3], to_core)

    def have(kind, j):
        for i, block in parts(kind, j):
            for slot in range(4):
                arrived(block(from_core[slot]), core_sem.at[i, slot])

    def load(kind, j, slot):
        have(kind, j)
        i = index(kind, j)
        own_block(kind, j, lambda src: pltpu.make_async_copy(src, w_s.at[slot, me], load_sem.at[slot]).start())
        for far_off in range(1, n):
            s = lax.rem(me + far_off, n)
            pltpu.make_async_copy(got.at[i, s], w_s.at[slot, s], load_sem.at[slot]).start()

    def loaded(slot):
        arrived(w_s.at[slot], load_sem.at[slot])

    rows = tokens // 2

    def product(lhs, slot):
        def some(r, _):
            here = pl.ds(pl.multiple_of(r * rows, rows), rows)
            acc_s[here, :] = jnp.dot(lhs[here, :], w_s[slot].reshape(n * B, B), preferred_element_type=jnp.float32)
        lax.fori_loop(0, 2, some, None)

    def turned(h):
        t = acc_s[:, h * HEAD : (h + 1) * HEAD].astype(jnp.bfloat16).astype(jnp.float32)
        return (t * cos_ref[...] + pltpu.roll(t, HEAD // 2, 1) * sin_ref[...]).astype(jnp.bfloat16)

    def norm():
        pltpu.make_async_copy(x_hbm, x_s, x_sem).start()
        arrived(x_s, x_sem)
        step = 32

        def some(r, _):
            here = pl.ds(pl.multiple_of(r * step, step), step)
            wide = x_s[here, :].astype(jnp.float32)
            scale = lax.rsqrt(jnp.mean(wide * wide, -1, keepdims=True) + 1e-6)
            a_s[here, :] = (wide * scale * gain_ref[...].astype(jnp.float32)).astype(jnp.bfloat16)
        lax.fori_loop(0, tokens // step, some, None)

    def make_kv():
        for j in (0, 1):
            load("w", j, piece("w", j))
        loaded(0)
        product(a_s, 0)
        for h in range(per):
            k_s[me, h] = turned(h)
        loaded(1)
        product(a_s, 1)
        for h in range(per):
            v_s[me, h] = acc_s[:, h * HEAD : (h + 1) * HEAD].astype(jnp.bfloat16).T

    e = HEAD**-0.5 * LOG2E

    def attend(p):
        kv_head = lax.div(p * per, group)
        for h in range(per):
            top_s[h : h + 1, :] = jnp.full((1, tokens), NEG, jnp.float32)
            mix_s[h] = jnp.zeros((HEAD + 8, tokens), jnp.float32)
        ones = jnp.ones((8, tokens), jnp.bfloat16)

        def block(b, masked):
            keys = k_s[b, kv_head]
            scores = [_dot(keys, q_s[h], 1, 1) for h in range(per)]
            if masked:
                shape = (tokens, tokens)
                ok = lax.broadcasted_iota(jnp.int32, shape, 1) >= lax.broadcasted_iota(jnp.int32, shape, 0)
            weights, keeps = [], []
            for h, s in enumerate(scores):
                if masked:
                    s = jnp.where(ok, s, HIDDEN)
                old = top_s[h : h + 1, :]
                top = jnp.maximum(old, s.max(axis=0, keepdims=True))
                top_s[h : h + 1, :] = top
                weights.append(jnp.exp2((s - top) * e).astype(jnp.bfloat16))
                keeps.append(jnp.exp2((old - top) * e))
            values = jnp.concatenate([v_s[b, kv_head], ones], axis=0)
            for h, (w, keep) in enumerate(zip(weights, keeps)):
                mix_s[h] = mix_s[h] * keep + _dot(values, w, 1, 0)

        lax.fori_loop(0, me, lambda b, _: block(b, False), None)
        block(me, True)
        for h in range(per):
            out = mix_s[h, :HEAD, :] * (1 / mix_s[h, HEAD : HEAD + 1, :])
            seen_s[:, pl.ds(pl.multiple_of(p * B + h * HEAD, HEAD), HEAD)] = out.T.astype(jnp.bfloat16)

    def pick(step, js, kind):
        got_j = js[0]
        for m, j in enumerate(js[1:], 1):
            got_j = lax.select(step == m, j, got_j)
        return got_j + odd * (pieces[kind] - 1 - 2 * got_j)

    acts = {"own": own, "near": near, "far": far, "have": have, "load": lambda kind, j: load(kind, j, 0)}

    def run(events):
        for what, *rest in events:
            {"norm": norm, "make_kv": make_kv, **acts}[what](*rest)

    barrier = pltpu.get_barrier_semaphore()
    partners = [to_right, to_left, to_core] + ([to_peer] if paired else [])
    for to in partners:
        pl.semaphore_signal(barrier, inc=1, device_id=to, device_id_type=MESH)
    pl.semaphore_wait(barrier, len(partners))

    run(BEFORE)

    def attend_step(step, _):
        slot = lax.rem(step, 2)
        for m, events in enumerate(DURING):
            pl.when(step == m)(functools.partial(run, events))
        loaded(slot)
        product(a_s, slot)
        for h in range(per):
            q_s[h] = turned(h)
        for m in range(len(ATTEND)):
            after = ("q", ATTEND[m + 1]) if m + 1 < len(ATTEND) else ("o", PROJECT[0])
            pl.when(step == m)(lambda m=m, after=after: load(*after, (m + 1) % 2))
        attend(pick(step, ATTEND, "q"))

    lax.fori_loop(0, len(ATTEND), attend_step, None)

    def columns(p):
        return pl.ds(pl.multiple_of(p * B, B), B)

    def project_step(step, _):
        slot = lax.rem(step + len(ATTEND), 2)
        p = pick(step, PROJECT, "o")
        for m, events in enumerate(AFTER):
            if events:
                pl.when(step == m)(functools.partial(run, events))
        loaded(slot)
        product(seen_s, slot)

        @pl.when(step >= 2)
        def _():
            arrived(y_s.at[slot], y_sem.at[slot])

        y_s[slot] = (x_s[:, columns(p)].astype(jnp.float32) + acc_s[...]).astype(jnp.bfloat16)
        pltpu.make_async_copy(y_s.at[slot], y_hbm.at[:, columns(p)], y_sem.at[slot]).start()
        for m in range(len(PROJECT) - 1):
            pl.when(step == m)(lambda m=m: load("o", PROJECT[m + 1], (len(ATTEND) + m + 1) % 2))

    lax.fori_loop(0, len(PROJECT), project_step, None)
    for slot in (0, 1):
        arrived(y_s.at[slot], y_sem.at[slot])

    for kind in ("w", "q", "o"):
        for j in range(pieces[kind]):
            if exported(kind, j):
                sent = got.at[pl.ds(0, 2), pl.ds(0, 5)]
            else:
                sent = got.at[0, pl.ds(0, 7 if along_x(kind, j) else 4)]
            arrived(sent, send_sem.at[index(kind, j)])
    arrived(k_s.at[pl.ds(0, 7)], send_sem.at[at_k])
    arrived(v_s.at[pl.ds(0, 7)], send_sem.at[at_k + 1])


def solution(mesh):
    n = mesh.shape["sp"]
    paired = mesh.shape["dp"] % 2 == 0

    def step(x, gain, wq, wk, wv, wo):
        tokens, width = x.shape
        place = lax.axis_index("sp") * tokens + jnp.arange(tokens)
        half = HEAD // 2
        angle = place.astype(jnp.float32)[:, None] * THETA ** (-jnp.arange(half, dtype=jnp.float32) / half)
        cos, sin = jnp.cos(angle), jnp.sin(angle)
        cos, sin = jnp.concatenate([cos, cos], -1), jnp.concatenate([-sin, sin], -1)
        chunks = 2 + wq.shape[1] // B + wo.shape[1] // B
        heads = wk.shape[1] // HEAD
        bf = jnp.bfloat16
        anywhere, vmem = pl.BlockSpec(memory_space=pl.ANY), pl.BlockSpec(memory_space=pltpu.VMEM)
        y, _ = pl.pallas_call(
            functools.partial(_kernel, n, paired),
            out_shape=[jax.ShapeDtypeStruct(x.shape, bf), jax.ShapeDtypeStruct((chunks, n, B, B), bf)],
            in_specs=[anywhere, vmem, anywhere, anywhere, anywhere, anywhere, vmem, vmem],
            out_specs=[anywhere, anywhere],
            scratch_shapes=[
                pltpu.VMEM((tokens, width), bf),
                pltpu.VMEM((tokens, width), bf),
                pltpu.VMEM((tokens, width), bf),
                pltpu.VMEM((n, heads, tokens, HEAD), bf),
                pltpu.VMEM((n, heads, HEAD, tokens), bf),
                pltpu.VMEM((2, n, B, B), bf),
                pltpu.VMEM((B // HEAD, tokens, HEAD), bf),
                pltpu.VMEM((tokens, B), jnp.float32),
                pltpu.VMEM((B // HEAD, tokens), jnp.float32),
                pltpu.VMEM((B // HEAD, HEAD + 8, tokens), jnp.float32),
                pltpu.VMEM((2, tokens, B), bf),
                pltpu.SemaphoreType.DMA((chunks + 2, 3)),
                pltpu.SemaphoreType.DMA((chunks + 2, 4)),
                pltpu.SemaphoreType.DMA((chunks + 2,)),
                pltpu.SemaphoreType.DMA((2,)),
                pltpu.SemaphoreType.DMA,
                pltpu.SemaphoreType.DMA((2,)),
            ],
            compiler_params=pltpu.CompilerParams(collective_id=0, has_side_effects=True, vmem_limit_bytes=VMEM),
        )(x, gain.reshape(1, -1), wq, wk, wv, wo, cos, sin)
        return y

    tokens, whole = P(("dp", "sp"), None), P("sp", None)
    return jax.shard_map(
        step,
        mesh=mesh,
        in_specs=(tokens, P(None), whole, whole, whole, whole),
        out_specs=tokens,
        check_vma=False,
    )
```

```python
import functools

import jax
import jax.numpy as jnp
import numpy as np
from jax import lax
from jax.experimental import pallas as pl
from jax.experimental.pallas import tpu as pltpu
from jax.sharding import PartitionSpec as P

HEAD = 128
THETA = 10000
NEG = -1e30
HIDDEN = 2 * NEG
LOG2E = 1.4426950408889634
VMEM = 58 * 2**20
MESH = pl.DeviceIdType.MESH
WIDTH = {"w": 256, "q": 512, "o": 256}
SHARED = {"w": 0, "q": 0, "o": 4}
SLOTS = 4

PLAN = [
    ("own", "w0"), ("own", "o15"), ("own", "o0"), ("own", "w1"), ("state", ""), ("own", "o12"), ("own", "o13"), ("angles", ""),
    ("near", "w0"), ("near", "w1"), ("own", "q1"), ("far", "w0"), ("load", "w0"), ("far", "w1"), ("load", "w1"), ("W", "w0"),
    ("own", "kv"), ("own", "q2"), ("near", "q1"), ("near", "kv"), ("near", "q2"), ("far", "q1"), ("load", "q1"), ("Q", "q1"),
    ("far", "kv"), ("own", "q0"), ("have", "kv"), ("A", "q1"), ("near", "o0"), ("far", "q2"), ("own", "o3"), ("own", "o1"),
    ("load", "q2"), ("near", "q0"), ("Q", "q2"), ("take", ""), ("V", "w0"), ("far", "o0"), ("own", "pv"), ("A", "q2"),
    ("near", "o1"), ("near", "o3"), ("near", "o15"), ("R", "q1"), ("R", "q2"), ("far", "o15"), ("far", "q0"), ("load", "q0"),
    ("Q", "q0"), ("near", "pv"), ("own", "o6"), ("A", "q0"), ("near", "o14"), ("far", "o1"), ("far", "o3"), ("R", "q0"),
    ("near", "o12"), ("far", "pv"), ("own", "q3"), ("near", "o6"), ("have", "pv"), ("B", "q1"), ("give", "q1"), ("far", "o12"),
    ("far", "o14"), ("own", "o8"), ("B", "q2"), ("give", "q2"), ("near", "q3"), ("near", "o8"), ("far", "o6"), ("own", "o10"),
    ("B", "q0"), ("give", "q0"), ("far", "q3"), ("own", "o2"), ("load", "q3"), ("load", "o0"), ("load", "o1"), ("load", "o15"),
    ("far", "o8"), ("Q", "q3"), ("near", "o10"), ("own", "o7"), ("A", "q3"), ("near", "o2"), ("far", "o10"), ("own", "o9"),
    ("load", "o3"), ("R", "q3"), ("near", "o7"), ("load", "o6"), ("B", "q3"), ("give", "q3"), ("near", "o9"), ("near", "o13"),
    ("far", "o2"), ("far", "o7"), ("own", "o11"), ("own", "o14"), ("own", "o5"), ("own", "o4"), ("load", "o2"), ("load", "o7"),
    ("load", "o14"), ("far", "o9"), ("near", "o11"), ("seen", ""), ("O", "o0"), ("load", "o8"), ("load", "o9"), ("O", "o14"),
    ("near", "o5"), ("far", "o13"), ("load", "o10"), ("O", "o2"), ("near", "o4"), ("load", "o12"), ("load", "o13"), ("O", "o6"),
    ("far", "o11"), ("O", "o8"), ("far", "o5"), ("load", "o11"), ("O", "o12"), ("far", "o4"), ("load", "o5"), ("O", "o10"),
    ("load", "o4"), ("O", "o4"),
]


def _dot(a, b, ca, cb):
    return lax.dot_general(a, b, (((ca,), (cb,)), ((), ())), preferred_element_type=jnp.float32)


def _kernel(n, x_hbm, gain_ref, wq, wk, wv, wo, freq_ref, y_ref, got_w, got_q, got_o,
            x_s, left_s, out_s, k_s, v_s, w_s, q_s, acc_s, top_s, prev_s, mix_s, score_s, cos_s, sin_s,
            near_sem, core_sem, send_sem, load_sem, x_sem, state_sem, give_sem, seen_sem):
    tokens, width = x_s.shape
    got = {"w": got_w, "q": got_q, "o": got_o}
    pieces = {kind: got[kind].shape[0] for kind in got}
    base = {"w": 0, "q": pieces["w"], "o": pieces["w"] + pieces["q"]}
    at_k = sum(pieces.values())
    depth = wq.shape[0]
    per = WIDTH["q"] // HEAD
    group = width // HEAD // (wk.shape[1] // HEAD)

    me = lax.axis_index("sp")
    dp = lax.axis_index("dp")
    side = lax.rem(me, 2)
    odd = lax.rem(dp, 2)
    right, left, opp = lax.rem(me + 2, n), lax.rem(me + n - 2, n), lax.rem(me + n // 2, n)
    core = me + 1 - 2 * side
    from_near = (left, right, opp)
    from_core = (core, lax.rem(core + n - 2, n), lax.rem(core + 2, n), lax.rem(core + n // 2, n))
    to_right, to_left, to_core = {"sp": right}, {"sp": left}, {"sp": core}
    to_peer = {"dp": dp + 1 - 2 * odd}
    onward = lax.select(side == 0, right, left)
    carried = lax.select(side == 0, left, right)

    def piece(kind, j):
        return j + odd * (pieces[kind] - 1 - 2 * j) if kind == "o" else j

    def index(kind, j):
        return base[kind] + piece(kind, j)

    def along_x(kind, j):
        return j < pieces[kind] - SHARED[kind]

    def exported(kind, j):
        return j < SHARED[kind]

    def own_block(kind, j, act):
        ref = {"w": (wk, wv)[j % 2], "q": wq, "o": wo}[kind]
        at = {"w": odd, "q": odd * pieces["q"] + j, "o": piece(kind, j)}[kind]
        act(ref.at[:, pl.ds(pl.multiple_of(at * WIDTH[kind], WIDTH[kind]), WIDTH[kind])])

    def send(src, dst, send_at, recv, to):
        pltpu.make_async_remote_copy(src_ref=src, dst_ref=dst, send_sem=send_sem.at[send_at], recv_sem=recv, device_id=to,
                                     device_id_type=MESH).start()

    def arrived(ref, sem):
        pltpu.make_async_copy(ref, ref, sem).wait()

    def parts(kind, j):
        if kind in ("kv", "pv"):
            seq = ("kv", "pv").index(kind)
            return [(at_k + 2 * seq, lambda s: k_s.at[seq, s]), (at_k + 2 * seq + 1, lambda s: v_s.at[seq, s])]
        p = piece(kind, j)
        return [(base[kind] + p, lambda s: got[kind].at[p, s])]

    def own(kind, j):
        def act(src, i, block):
            if kind in ("kv", "pv") or along_x(kind, j):
                send(src, block(me), i, near_sem.at[i, 0], to_right)
                send(src, block(me), i, near_sem.at[i, 1], to_left)
            send(src, block(me), i, core_sem.at[i, 0], to_core)

        for i, block in parts(kind, j):
            if kind in ("kv", "pv"):
                act(block(me), i, block)
            else:
                own_block(kind, j, lambda src: act(src, i, block))

    def near(kind, j):
        for i, block in parts(kind, j):
            for slot in (0, 1):
                s = from_near[slot]
                arrived(block(s), near_sem.at[i, slot])
                if kind == "o" and exported(kind, j):
                    send(block(s), block(s), i, near_sem.at[i, slot], to_peer)
            if kind in ("kv", "pv") or along_x(kind, j):
                send(block(carried), block(carried), i, near_sem.at[i, 2], {"sp": onward})
            for slot in (0, 1):
                s = from_near[slot]
                send(block(s), block(s), i, core_sem.at[i, 1 + slot], to_core)

    def far(kind, j):
        for i, block in parts(kind, j):
            arrived(block(opp), near_sem.at[i, 2])
            if kind == "o" and exported(kind, j):
                send(block(opp), block(opp), i, near_sem.at[i, 2], to_peer)
            send(block(opp), block(opp), i, core_sem.at[i, 3], to_core)

    def have(kind, j):
        for i, block in parts(kind, j):
            for slot in range(4):
                arrived(block(from_core[slot]), core_sem.at[i, slot])

    def load(kind, j, slot):
        have(kind, j)
        p = piece(kind, j)
        b = WIDTH[kind]
        half = pl.ds(pl.multiple_of(lax.rem(p, WIDTH["q"] // b) * b, b), b)
        own_block(kind, j, lambda src: pltpu.make_async_copy(src, w_s.at[slot, me, :, half], load_sem.at[slot]).start())
        for far_off in range(1, n):
            s = lax.rem(me + far_off, n)
            pltpu.make_async_copy(got[kind].at[p, s], w_s.at[slot, s, :, half], load_sem.at[slot]).start()

    rows = tokens // 2

    def product(which, slot):
        def some(r, _):
            here = pl.ds(pl.multiple_of(r * rows, rows), rows)
            acc_s[here, :] = jnp.dot(left_s[which, here, :], w_s[slot].reshape(n * depth, WIDTH["q"]), preferred_element_type=jnp.float32)
        lax.fori_loop(0, 2, some, None)

    def turned(h):
        t = acc_s[:, h * HEAD : (h + 1) * HEAD].astype(jnp.bfloat16).astype(jnp.float32)
        return (t * cos_s[...] + pltpu.roll(t, HEAD // 2, 1) * sin_s[...]).astype(jnp.bfloat16)

    def norm():
        arrived(x_s, x_sem)
        step = 32

        def some(r, _):
            here = pl.ds(pl.multiple_of(r * step, step), step)
            wide = x_s[here, :].astype(jnp.float32)
            scale = lax.rsqrt(jnp.mean(wide * wide, -1, keepdims=True) + 1e-6)
            left_s[0, here, :] = (wide * scale * gain_ref[...].astype(jnp.float32)[None]).astype(jnp.bfloat16)
        lax.fori_loop(0, tokens // step, some, None)

    def angles():
        step = 128

        def some(r, _):
            here = pl.ds(pl.multiple_of(r * step, step), step)
            place = me * tokens + r * step + lax.broadcasted_iota(jnp.int32, (step, HEAD), 0)
            angle = place.astype(jnp.float32) * freq_ref[...]
            cos_s[here, :] = jnp.cos(angle)
            sin = jnp.sin(angle)
            sin_s[here, :] = jnp.where(lax.broadcasted_iota(jnp.int32, (step, HEAD), 1) < HEAD // 2, -sin, sin)
        lax.fori_loop(0, tokens // step, some, None)

    e = HEAD**-0.5 * LOG2E

    def attend(seq, p):
        kv_head = lax.div(p * per, group)
        for h in range(per):
            top_s[h : h + 1, :] = jnp.full((1, tokens), NEG, jnp.float32)
            mix_s[h] = jnp.zeros((HEAD + 8, tokens), jnp.float32)

        def score(b, h, masked):
            s = _dot(k_s[seq, b, kv_head], q_s[seq, p, h], 1, 1)
            if masked:
                shape = (tokens, tokens)
                s = jnp.where(lax.broadcasted_iota(jnp.int32, shape, 1) >= lax.broadcasted_iota(jnp.int32, shape, 0), s, HIDDEN)
            old = top_s[h : h + 1, :]
            prev_s[h : h + 1, :] = old
            top_s[h : h + 1, :] = jnp.maximum(old, s.max(axis=0, keepdims=True))
            score_s[h] = s

        def weigh(b, coming):
            values = jnp.concatenate([v_s[seq, b, kv_head], jnp.ones((8, tokens), jnp.bfloat16)], axis=0)
            for h in range(per):
                top = top_s[h : h + 1, :]
                weights = jnp.exp2((score_s[h] - top) * e).astype(jnp.bfloat16)
                keep = jnp.exp2((prev_s[h : h + 1, :] - top) * e)
                if coming is not None:
                    score(coming, h, False)
                mix_s[h] = mix_s[h] * keep + _dot(values, weights, 1, 0)

        for h in range(per):
            score(me, h, True)
        lax.fori_loop(0, me, lambda b, _: weigh(lax.select(b == 0, me, b - 1), b), None)
        weigh(lax.select(me == 0, me, me - 1), None)
        for h in range(per):
            out = mix_s[h, :HEAD, :] * (1 / mix_s[h, HEAD : HEAD + 1, :])
            out_s[p, :, h * HEAD : (h + 1) * HEAD] = out.T.astype(jnp.bfloat16)

        @pl.when(seq == 0)
        def _():
            left_s[1, :, mine(p)] = out_s[p]

    def mine(p):
        b = WIDTH["q"]
        return pl.ds(pl.multiple_of((odd * pieces["q"] + p) * b, b), b)

    def give(p):
        pltpu.make_async_remote_copy(src_ref=out_s.at[p], dst_ref=left_s.at[1, :, mine(p)], send_sem=give_sem.at[p], recv_sem=seen_sem.at[p],
                                     device_id=to_peer, device_id_type=MESH).start()

    def seen():
        for p in range(pieces["q"]):
            arrived(out_s.at[p], seen_sem.at[p])

    def project(p):
        b = WIDTH["q"]
        at = pl.ds(pl.multiple_of(lax.div(p, 2) * b, b), b)
        y_ref[:, at] = (x_s[:, at].astype(jnp.float32) + acc_s[...]).astype(jnp.bfloat16)

    def keys(seq):
        heads = WIDTH["w"] // HEAD
        for h in range(heads):
            k_s[seq, me, h] = turned(h)
            v_s[seq, me, h] = acc_s[:, (heads + h) * HEAD : (heads + h + 1) * HEAD].astype(jnp.bfloat16).T

    def queries(seq, p):
        for h in range(per):
            q_s[seq, p, h] = turned(h)

    pltpu.make_async_copy(x_hbm, x_s, x_sem).start()
    barrier = pltpu.get_barrier_semaphore()
    partners = [to_right, to_left, to_core, to_peer]

    for to in partners:
        pl.semaphore_signal(barrier, inc=1, device_id=to, device_id_type=MESH)

    names = "WVQRABO"
    steps, events, slots, place = [], [], [], {}
    for what, token in PLAN:
        kind, j = (token, 0) if not token[-1:].isdigit() else (token[0], int(token[1:]))
        key = (kind, j if kind == "q" else j // 2)
        if what in names:
            steps.append((what, kind, j, events))
            slots.append(place.get(key, 0))
            events = []
        else:
            if what == "load" and key not in place:
                place[key] = len(place) % SLOTS
            events.append((what, kind, j, place.get(key, 0)))
    tail = events
    acts = {"own": own, "near": near, "far": far, "have": have}

    def run(events):
        for what, kind, j, slot in events:
            with jax.named_scope(f"{what}_{kind}_{j}"):
                if what == "angles":
                    angles()
                elif what == "state":
                    norm()
                    pltpu.make_async_remote_copy(src_ref=left_s.at[0], dst_ref=left_s.at[2], send_sem=state_sem.at[0], recv_sem=state_sem.at[1],
                                                 device_id=to_peer, device_id_type=MESH).start()
                elif what == "take":
                    arrived(left_s.at[2], state_sem.at[1])
                elif what == "give":
                    give(j)
                elif what == "seen":
                    seen()
                elif what == "load":
                    load(kind, j, slot)
                else:
                    acts[what](kind, j)

    def pick(step, values, first=0):
        if len(set(values)) == 1:
            return jnp.int32(values[0])
        half = len(values) // 2
        return jnp.where(step < first + half, pick(step, values[:half], first), pick(step, values[half:], first + half))

    def choose(step, first, end):
        if not any(steps[m][3] for m in range(first, end)):
            return
        if end - first == 1:
            run(steps[first][3])
            return
        half = (first + end) // 2
        pl.when(step < half)(lambda: choose(step, first, half))
        pl.when(step >= half)(lambda: choose(step, half, end))

    def go(step, _):
        choose(step, 0, len(steps))
        code = pick(step, [names.index(what) + 8 * (slot + 8 * j) for (what, _, j, _), slot in zip(steps, slots)])
        what, slot, j = code & 7, (code >> 3) & 7, code >> 6
        seq = what & 1
        p = jnp.where(what == 6, j + odd * (pieces["o"] - 1 - 2 * j), j)
        state = 2 * seq

        @pl.when((what < 4) | (what == 6))
        def _():
            with jax.named_scope("wait"):
                pl.when((what & 1) == 0)(lambda: arrived(w_s.at[slot], load_sem.at[slot]))
            with jax.named_scope("product"):
                product(jnp.where(what == 6, 1, state), slot)
                pl.when(what < 2)(lambda: keys(seq))
                pl.when((what == 2) | (what == 3))(lambda: queries(seq, p))
                pl.when(what == 6)(lambda: project(p))

        @pl.when((what == 4) | (what == 5))
        def _():
            with jax.named_scope("attend"):
                attend(seq, p)

    with jax.named_scope("barrier"):
        pl.semaphore_wait(barrier, len(partners))

    lax.fori_loop(0, len(steps), go, None)
    run(tail)

    for kind in ("w", "q", "o"):
        for j in range(pieces[kind]):
            if exported(kind, j):
                sent = got[kind].at[pl.ds(0, 2), pl.ds(0, 5)]
            else:
                sent = got[kind].at[0, pl.ds(0, 7 if along_x(kind, j) else 4)]
            arrived(sent, send_sem.at[index(kind, j)])
    for seq in range(2):
        arrived(k_s.at[seq, pl.ds(0, 7)], send_sem.at[at_k + 2 * seq])
        arrived(v_s.at[seq, pl.ds(0, 7)], send_sem.at[at_k + 2 * seq + 1])
    arrived(left_s.at[0], state_sem.at[0])
    for p in range(pieces["q"]):
        arrived(out_s.at[p], give_sem.at[p])


def solution(mesh):
    n = mesh.shape["sp"]

    def step(x, gain, wq, wk, wv, wo):
        tokens, width = x.shape
        half = HEAD // 2
        freq = np.float32(THETA) ** (-np.arange(half, dtype=np.float32) / np.float32(half))
        freq = jnp.asarray(np.concatenate([freq, freq])[None])
        pieces = {"w": wk.shape[1] // WIDTH["w"], "q": wq.shape[1] // WIDTH["q"] // 2, "o": wo.shape[1] // WIDTH["o"]}
        got = {kind: (pieces[kind], n, wq.shape[0], WIDTH[kind]) for kind in pieces}
        chunks = sum(pieces.values())
        per = WIDTH["q"] // HEAD
        heads = wk.shape[1] // HEAD // 2
        bf = jnp.bfloat16
        anywhere, vmem = pl.BlockSpec(memory_space=pl.ANY), pl.BlockSpec(memory_space=pltpu.VMEM)
        y, *_ = pl.pallas_call(
            functools.partial(_kernel, n),
            out_shape=[pltpu.VMEM(x.shape, bf), *(jax.ShapeDtypeStruct(got[kind], bf) for kind in "wqo")],
            in_specs=[anywhere, vmem, anywhere, anywhere, anywhere, anywhere, vmem],
            out_specs=[vmem, anywhere, anywhere, anywhere],
            scratch_shapes=[
                pltpu.VMEM((tokens, width), bf),
                pltpu.VMEM((3, tokens, width), bf),
                pltpu.VMEM((pieces["q"], tokens, WIDTH["q"]), bf),
                pltpu.VMEM((2, n, heads, tokens, HEAD), bf),
                pltpu.VMEM((2, n, heads, HEAD, tokens), bf),
                pltpu.VMEM((SLOTS, *got["q"][1:]), bf),
                pltpu.VMEM((2, pieces["q"], per, tokens, HEAD), bf),
                pltpu.VMEM((tokens, WIDTH["q"]), jnp.float32),
                pltpu.VMEM((per, tokens), jnp.float32),
                pltpu.VMEM((per, tokens), jnp.float32),
                pltpu.VMEM((per, HEAD + 8, tokens), jnp.float32),
                pltpu.VMEM((per, tokens, tokens), jnp.float32),
                pltpu.VMEM((tokens, HEAD), jnp.float32),
                pltpu.VMEM((tokens, HEAD), jnp.float32),
                pltpu.SemaphoreType.DMA((chunks + 4, 3)),
                pltpu.SemaphoreType.DMA((chunks + 4, 4)),
                pltpu.SemaphoreType.DMA((chunks + 4,)),
                pltpu.SemaphoreType.DMA((SLOTS,)),
                pltpu.SemaphoreType.DMA,
                pltpu.SemaphoreType.DMA((2,)),
                pltpu.SemaphoreType.DMA((pieces["q"],)),
                pltpu.SemaphoreType.DMA((pieces["q"],)),
            ],
            compiler_params=pltpu.CompilerParams(collective_id=0, has_side_effects=True, vmem_limit_bytes=VMEM),
        )(x, gain, wq, wk, wv, wo, freq)
        return y

    tokens, whole = P(("dp", "sp"), None), P("sp", None)
    return jax.shard_map(
        step,
        mesh=mesh,
        in_specs=(tokens, P(None), whole, whole, whole, whole),
        out_specs=tokens,
        check_vma=False,
    )
```

```python
import functools

import jax
import jax.numpy as jnp
import numpy as np
from jax import lax
from jax.experimental import pallas as pl
from jax.experimental.pallas import tpu as pltpu
from jax.sharding import PartitionSpec as P

HEAD = 128
THETA = 10000
NEG = -1e30
HIDDEN = 2 * NEG
LOG2E = 1.4426950408889634
VMEM = 58 * 2**20
MESH = pl.DeviceIdType.MESH
WIDTH = {"w": 256, "q": 512, "o": 256}
SHARED = {"w": 0, "q": 0, "o": 4}
PARTLY = 1
SLOTS = 4

PLAN = [
    ("own", "w0"), ("own", "o15"), ("own", "o13"), ("angles", ""), ("own", "q3"), ("own", "w1"), ("state", ""), ("near", "w0"),
    ("near", "q3"), ("near", "w1"), ("far", "w0"), ("load", "w0"), ("far", "q3"), ("own", "q0"), ("load", "q3"), ("far", "w1"),
    ("Q", "q3"), ("load", "w1"), ("W", "w0"), ("own", "kv"), ("near", "q0"), ("near", "kv"), ("far", "q0"), ("own", "q2"),
    ("load", "q0"), ("Q", "q0"), ("far", "kv"), ("own", "o0"), ("have", "kv"), ("A", "q3"), ("near", "q2"), ("own", "o1"),
    ("own", "o2"), ("A", "q0"), ("near", "o0"), ("take", ""), ("V", "w0"), ("far", "q2"), ("own", "pv"), ("R", "q3"),
    ("near", "o1"), ("load", "q2"), ("R", "q0"), ("near", "o2"), ("Q", "q2"), ("near", "o15"), ("R", "q2"), ("far", "o0"),
    ("A", "q2"), ("near", "o14"), ("near", "pv"), ("far", "o1"), ("own", "q1"), ("own", "o11"), ("far", "o2"), ("near", "o13"),
    ("far", "pv"), ("own", "o4"), ("far", "o15"), ("have", "pv"), ("B", "q3"), ("give", "q3"), ("near", "q1"), ("far", "o14"),
    ("own", "o8"), ("own", "o12"), ("own", "o14"), ("own", "o9"), ("B", "q0"), ("give", "q0"), ("near", "o4"), ("near", "o11"),
    ("far", "o13"), ("B", "q2"), ("give", "q2"), ("near", "o8"), ("far", "q1"), ("own", "o10"), ("own", "o3"), ("near", "o9"),
    ("load", "q1"), ("load", "o0"), ("load", "o1"), ("load", "o14"), ("load", "o15"), ("Q", "q1"), ("far", "o4"), ("R", "q1"),
    ("B", "q1"), ("give", "q1"), ("near", "o3"), ("near", "o10"), ("far", "o8"), ("own", "o5"), ("own", "o7"), ("own", "o6"),
    ("load", "o2"), ("A", "q1"), ("far", "o3"), ("far", "o9"), ("far", "o11"), ("load", "o8"), ("load", "o3"), ("load", "o9"),
    ("far", "o10"), ("seen", ""), ("O", "o0"), ("load", "o10"), ("load", "o11"), ("O", "o14"), ("near", "o5"), ("load", "o4"),
    ("O", "o2"), ("near", "o7"), ("O", "o8"), ("near", "o6"), ("near", "o12"), ("load", "o13"), ("O", "o10"), ("far", "o5"),
    ("load", "o5"), ("far", "o7"), ("far", "o12"), ("O", "o4"), ("far", "o6"), ("load", "o7"), ("load", "o12"), ("load", "o6"),
    ("O", "o12"), ("O", "o6"),
]


def _dot(a, b, ca, cb):
    return lax.dot_general(a, b, (((ca,), (cb,)), ((), ())), preferred_element_type=jnp.float32)


def _kernel(n, x_hbm, gain_ref, wq, wk, wv, wo, freq_ref, y_ref, got_w, got_q, got_o,
            x_s, left_s, out_s, k_s, v_s, w_s, q_s, acc_s, top_s, prev_s, mix_s, score_s, cos_s, sin_s,
            near_sem, core_sem, send_sem, load_sem, x_sem, state_sem, give_sem, seen_sem):
    tokens, width = x_s.shape
    got = {"w": got_w, "q": got_q, "o": got_o}
    pieces = {kind: got[kind].shape[0] for kind in got}
    base = {"w": 0, "q": pieces["w"], "o": pieces["w"] + pieces["q"]}
    at_k = sum(pieces.values())
    depth = wq.shape[0]
    per = WIDTH["q"] // HEAD
    group = width // HEAD // (wk.shape[1] // HEAD)

    me = lax.axis_index("sp")
    dp = lax.axis_index("dp")
    side = lax.rem(me, 2)
    odd = lax.rem(dp, 2)
    right, left, opp = lax.rem(me + 2, n), lax.rem(me + n - 2, n), lax.rem(me + n // 2, n)
    core = me + 1 - 2 * side
    from_near = (left, right, opp)
    from_core = (core, lax.rem(core + n - 2, n), lax.rem(core + 2, n), lax.rem(core + n // 2, n))
    to_right, to_left, to_core = {"sp": right}, {"sp": left}, {"sp": core}
    to_peer = {"dp": dp + 1 - 2 * odd}
    onward = lax.select(side == 0, right, left)
    carried = lax.select(side == 0, left, right)

    def piece(kind, j):
        return j + odd * (pieces[kind] - 1 - 2 * j) if kind == "o" else j

    def index(kind, j):
        return base[kind] + piece(kind, j)

    def along_x(kind, j):
        return j < pieces[kind] - SHARED[kind]

    def exported(kind, j):
        return j < SHARED[kind]

    def far_exported(kind, j):
        return kind == "o" and j < SHARED[kind] + PARTLY

    def relayed(kind, j):
        return kind != "o" or j < pieces[kind] - SHARED[kind] - PARTLY

    def own_block(kind, j, act):
        ref = {"w": (wk, wv)[j % 2], "q": wq, "o": wo}[kind]
        at = {"w": odd, "q": odd * pieces["q"] + j, "o": piece(kind, j)}[kind]
        act(ref.at[:, pl.ds(pl.multiple_of(at * WIDTH[kind], WIDTH[kind]), WIDTH[kind])])

    def send(src, dst, send_at, recv, to):
        pltpu.make_async_remote_copy(src_ref=src, dst_ref=dst, send_sem=send_sem.at[send_at], recv_sem=recv, device_id=to,
                                     device_id_type=MESH).start()

    def arrived(ref, sem):
        pltpu.make_async_copy(ref, ref, sem).wait()

    def parts(kind, j):
        if kind in ("kv", "pv"):
            seq = ("kv", "pv").index(kind)
            return [(at_k + 2 * seq, lambda s: k_s.at[seq, s]), (at_k + 2 * seq + 1, lambda s: v_s.at[seq, s])]
        p = piece(kind, j)
        return [(base[kind] + p, lambda s: got[kind].at[p, s])]

    def own(kind, j):
        def act(src, i, block):
            if kind in ("kv", "pv") or along_x(kind, j):
                send(src, block(me), i, near_sem.at[i, 0], to_right)
                send(src, block(me), i, near_sem.at[i, 1], to_left)
            send(src, block(me), i, core_sem.at[i, 0], to_core)

        for i, block in parts(kind, j):
            if kind in ("kv", "pv"):
                act(block(me), i, block)
            else:
                own_block(kind, j, lambda src: act(src, i, block))

    def near(kind, j):
        for i, block in parts(kind, j):
            for slot in (0, 1):
                s = from_near[slot]
                arrived(block(s), near_sem.at[i, slot])
                if kind == "o" and exported(kind, j):
                    send(block(s), block(s), i, near_sem.at[i, slot], to_peer)
            if relayed(kind, j):
                send(block(carried), block(carried), i, near_sem.at[i, 2], {"sp": onward})
            for slot in (0, 1):
                s = from_near[slot]
                send(block(s), block(s), i, core_sem.at[i, 1 + slot], to_core)

    def far(kind, j):
        for i, block in parts(kind, j):
            arrived(block(opp), near_sem.at[i, 2])
            if far_exported(kind, j):
                send(block(opp), block(opp), i, near_sem.at[i, 2], to_peer)
            send(block(opp), block(opp), i, core_sem.at[i, 3], to_core)

    def have(kind, j):
        for i, block in parts(kind, j):
            for slot in range(4):
                arrived(block(from_core[slot]), core_sem.at[i, slot])

    def load(kind, j, slot):
        have(kind, j)
        p = piece(kind, j)
        b = WIDTH[kind]
        half = pl.ds(pl.multiple_of(lax.rem(p, WIDTH["q"] // b) * b, b), b)
        own_block(kind, j, lambda src: pltpu.make_async_copy(src, w_s.at[slot, me, :, half], load_sem.at[slot]).start())
        for far_off in range(1, n):
            s = lax.rem(me + far_off, n)
            pltpu.make_async_copy(got[kind].at[p, s], w_s.at[slot, s, :, half], load_sem.at[slot]).start()

    rows = tokens // 2

    def product(which, slot):
        def some(r, _):
            here = pl.ds(pl.multiple_of(r * rows, rows), rows)
            acc_s[here, :] = jnp.dot(left_s[which, here, :], w_s[slot].reshape(n * depth, WIDTH["q"]), preferred_element_type=jnp.float32)
        lax.fori_loop(0, 2, some, None)

    def turned(h):
        t = acc_s[:, h * HEAD : (h + 1) * HEAD].astype(jnp.bfloat16).astype(jnp.float32)
        return (t * cos_s[...] + pltpu.roll(t, HEAD // 2, 1) * sin_s[...]).astype(jnp.bfloat16)

    parts_of_state = 4

    def quarter(r):
        size = tokens // parts_of_state
        return pl.ds(pl.multiple_of(r * size, size), size)

    def norm(first):
        step = 32

        def some(r, _):
            here = pl.ds(pl.multiple_of(first * (tokens // parts_of_state) + r * step, step), step)
            wide = x_s[here, :].astype(jnp.float32)
            scale = lax.rsqrt(jnp.mean(wide * wide, -1, keepdims=True) + 1e-6)
            left_s[0, here, :] = (wide * scale * gain_ref[...].astype(jnp.float32)[None]).astype(jnp.bfloat16)
        lax.fori_loop(0, tokens // parts_of_state // step, some, None)

    def states():
        arrived(x_s, x_sem)

        def some(r, _):
            norm(r)
            pltpu.make_async_remote_copy(src_ref=left_s.at[0, quarter(r)], dst_ref=left_s.at[2, quarter(r)], send_sem=state_sem.at[0, r],
                                         recv_sem=state_sem.at[1, r], device_id=to_peer, device_id_type=MESH).start()
        lax.fori_loop(0, parts_of_state, some, None)

    def angles():
        step = 128

        def some(r, _):
            here = pl.ds(pl.multiple_of(r * step, step), step)
            place = me * tokens + r * step + lax.broadcasted_iota(jnp.int32, (step, HEAD), 0)
            angle = place.astype(jnp.float32) * freq_ref[...]
            cos_s[here, :] = jnp.cos(angle)
            sin = jnp.sin(angle)
            sin_s[here, :] = jnp.where(lax.broadcasted_iota(jnp.int32, (step, HEAD), 1) < HEAD // 2, -sin, sin)
        lax.fori_loop(0, tokens // step, some, None)

    e = HEAD**-0.5 * LOG2E

    def attend(seq, p):
        kv_head = lax.div(p * per, group)
        for h in range(per):
            top_s[h : h + 1, :] = jnp.full((1, tokens), NEG, jnp.float32)
            mix_s[h] = jnp.zeros((HEAD + 8, tokens), jnp.float32)

        def score(b, h, masked):
            s = _dot(k_s[seq, b, kv_head], q_s[seq, p, h], 1, 1)
            if masked:
                shape = (tokens, tokens)
                s = jnp.where(lax.broadcasted_iota(jnp.int32, shape, 1) >= lax.broadcasted_iota(jnp.int32, shape, 0), s, HIDDEN)
            old = top_s[h : h + 1, :]
            prev_s[h : h + 1, :] = old
            top_s[h : h + 1, :] = jnp.maximum(old, s.max(axis=0, keepdims=True))
            score_s[h] = s

        def weigh(b, coming):
            values = jnp.concatenate([v_s[seq, b, kv_head], jnp.ones((8, tokens), jnp.bfloat16)], axis=0)
            for h in range(per):
                top = top_s[h : h + 1, :]
                weights = jnp.exp2((score_s[h] - top) * e).astype(jnp.bfloat16)
                keep = jnp.exp2((prev_s[h : h + 1, :] - top) * e)
                if coming is not None:
                    score(coming, h, False)
                mix_s[h] = mix_s[h] * keep + _dot(values, weights, 1, 0)

        for h in range(per):
            score(me, h, True)
        lax.fori_loop(0, me, lambda b, _: weigh(lax.select(b == 0, me, b - 1), b), None)
        weigh(lax.select(me == 0, me, me - 1), None)
        for h in range(per):
            out = mix_s[h, :HEAD, :] * (1 / mix_s[h, HEAD : HEAD + 1, :])
            out = out.T.astype(jnp.bfloat16)

            @pl.when(seq == 0)
            def _():
                left_s[1, :, pl.ds(pl.multiple_of(((odd * pieces["q"] + p) * per + h) * HEAD, HEAD), HEAD)] = out

            @pl.when(seq == 1)
            def _():
                out_s[p, :, h * HEAD : (h + 1) * HEAD] = out

    def mine(p):
        b = WIDTH["q"]
        return pl.ds(pl.multiple_of((odd * pieces["q"] + p) * b, b), b)

    def give(p):
        pltpu.make_async_remote_copy(src_ref=out_s.at[p], dst_ref=left_s.at[1, :, mine(p)], send_sem=give_sem.at[p], recv_sem=seen_sem.at[p],
                                     device_id=to_peer, device_id_type=MESH).start()

    def seen():
        for p in range(pieces["q"]):
            arrived(out_s.at[p], seen_sem.at[p])

    def project(p):
        b = WIDTH["q"]
        at = pl.ds(pl.multiple_of(lax.div(p, 2) * b, b), b)
        y_ref[:, at] = (x_s[:, at].astype(jnp.float32) + acc_s[...]).astype(jnp.bfloat16)

    def keys(seq):
        heads = WIDTH["w"] // HEAD
        for h in range(heads):
            k_s[seq, me, h] = turned(h)
            v_s[seq, me, h] = acc_s[:, (heads + h) * HEAD : (heads + h + 1) * HEAD].astype(jnp.bfloat16).T

    def queries(seq, p):
        for h in range(per):
            q_s[seq, p, h] = turned(h)

    pltpu.make_async_copy(x_hbm, x_s, x_sem).start()
    barrier = pltpu.get_barrier_semaphore()
    partners = [to_right, to_left, to_core, to_peer]

    for to in partners:
        pl.semaphore_signal(barrier, inc=1, device_id=to, device_id_type=MESH)

    names = "WVQRABO"
    steps, events, slots, place = [], [], [], {}
    for what, token in PLAN:
        kind, j = (token, 0) if not token[-1:].isdigit() else (token[0], int(token[1:]))
        key = (kind, j if kind == "q" else j // 2)
        if what in names:
            steps.append((what, kind, j, events))
            slots.append(place.get(key, 0))
            events = []
        else:
            if what == "load" and key not in place:
                place[key] = len(place) % SLOTS
            events.append((what, kind, j, place.get(key, 0)))
    tail = events
    acts = {"own": own, "near": near, "far": far, "have": have}

    def run(events):
        for what, kind, j, slot in events:
            with jax.named_scope(f"{what}_{kind}_{j}"):
                if what == "angles":
                    angles()
                elif what == "state":
                    states()
                elif what == "take":
                    for r in range(parts_of_state):
                        arrived(left_s.at[2, quarter(r)], state_sem.at[1, r])
                elif what == "give":
                    give(j)
                elif what == "seen":
                    seen()
                elif what == "load":
                    load(kind, j, slot)
                else:
                    acts[what](kind, j)

    def pick(step, values, first=0):
        if len(set(values)) == 1:
            return jnp.int32(values[0])
        half = len(values) // 2
        return jnp.where(step < first + half, pick(step, values[:half], first), pick(step, values[half:], first + half))

    def choose(step, first, end):
        if not any(steps[m][3] for m in range(first, end)):
            return
        if end - first == 1:
            run(steps[first][3])
            return
        half = (first + end) // 2
        pl.when(step < half)(lambda: choose(step, first, half))
        pl.when(step >= half)(lambda: choose(step, half, end))

    def go(step, _):
        choose(step, 0, len(steps))
        code = pick(step, [names.index(what) + 8 * (slot + 8 * j) for (what, _, j, _), slot in zip(steps, slots)])
        what, slot, j = code & 7, (code >> 3) & 7, code >> 6
        seq = what & 1
        p = jnp.where(what == 6, j + odd * (pieces["o"] - 1 - 2 * j), j)
        state = 2 * seq

        @pl.when((what < 4) | (what == 6))
        def _():
            with jax.named_scope("wait"):
                pl.when((what & 1) == 0)(lambda: arrived(w_s.at[slot], load_sem.at[slot]))
            with jax.named_scope("product"):
                product(jnp.where(what == 6, 1, state), slot)
                pl.when(what < 2)(lambda: keys(seq))
                pl.when((what == 2) | (what == 3))(lambda: queries(seq, p))
                pl.when(what == 6)(lambda: project(p))

        @pl.when((what == 4) | (what == 5))
        def _():
            with jax.named_scope("attend"):
                attend(seq, p)

    with jax.named_scope("barrier"):
        pl.semaphore_wait(barrier, len(partners))

    lax.fori_loop(0, len(steps), go, None)
    run(tail)

    for kind in ("w", "q", "o"):
        for j in range(pieces[kind]):
            count = 4 + 2 * along_x(kind, j) + relayed(kind, j) + 2 * exported(kind, j) + far_exported(kind, j)
            half = 2 - count % 2
            sent = got[kind].at[pl.ds(0, half), pl.ds(0, count // half)]
            arrived(sent, send_sem.at[index(kind, j)])
    for seq in range(2):
        arrived(k_s.at[seq, pl.ds(0, 7)], send_sem.at[at_k + 2 * seq])
        arrived(v_s.at[seq, pl.ds(0, 7)], send_sem.at[at_k + 2 * seq + 1])
    for r in range(parts_of_state):
        arrived(left_s.at[0, quarter(r)], state_sem.at[0, r])
    for p in range(pieces["q"]):
        arrived(out_s.at[p], give_sem.at[p])


def solution(mesh):
    n = mesh.shape["sp"]

    def step(x, gain, wq, wk, wv, wo):
        tokens, width = x.shape
        half = HEAD // 2
        freq = np.float32(THETA) ** (-np.arange(half, dtype=np.float32) / np.float32(half))
        freq = jnp.asarray(np.concatenate([freq, freq])[None])
        pieces = {"w": wk.shape[1] // WIDTH["w"], "q": wq.shape[1] // WIDTH["q"] // 2, "o": wo.shape[1] // WIDTH["o"]}
        got = {kind: (pieces[kind], n, wq.shape[0], WIDTH[kind]) for kind in pieces}
        chunks = sum(pieces.values())
        per = WIDTH["q"] // HEAD
        heads = wk.shape[1] // HEAD // 2
        bf = jnp.bfloat16
        anywhere, vmem = pl.BlockSpec(memory_space=pl.ANY), pl.BlockSpec(memory_space=pltpu.VMEM)
        y, *_ = pl.pallas_call(
            functools.partial(_kernel, n),
            out_shape=[pltpu.VMEM(x.shape, bf), *(jax.ShapeDtypeStruct(got[kind], bf) for kind in "wqo")],
            in_specs=[anywhere, vmem, anywhere, anywhere, anywhere, anywhere, vmem],
            out_specs=[vmem, anywhere, anywhere, anywhere],
            scratch_shapes=[
                pltpu.VMEM((tokens, width), bf),
                pltpu.VMEM((3, tokens, width), bf),
                pltpu.VMEM((pieces["q"], tokens, WIDTH["q"]), bf),
                pltpu.VMEM((2, n, heads, tokens, HEAD), bf),
                pltpu.VMEM((2, n, heads, HEAD, tokens), bf),
                pltpu.VMEM((SLOTS, *got["q"][1:]), bf),
                pltpu.VMEM((2, pieces["q"], per, tokens, HEAD), bf),
                pltpu.VMEM((tokens, WIDTH["q"]), jnp.float32),
                pltpu.VMEM((per, tokens), jnp.float32),
                pltpu.VMEM((per, tokens), jnp.float32),
                pltpu.VMEM((per, HEAD + 8, tokens), jnp.float32),
                pltpu.VMEM((per, tokens, tokens), jnp.float32),
                pltpu.VMEM((tokens, HEAD), jnp.float32),
                pltpu.VMEM((tokens, HEAD), jnp.float32),
                pltpu.SemaphoreType.DMA((chunks + 4, 3)),
                pltpu.SemaphoreType.DMA((chunks + 4, 4)),
                pltpu.SemaphoreType.DMA((chunks + 4,)),
                pltpu.SemaphoreType.DMA((SLOTS,)),
                pltpu.SemaphoreType.DMA,
                pltpu.SemaphoreType.DMA((2, 4)),
                pltpu.SemaphoreType.DMA((pieces["q"],)),
                pltpu.SemaphoreType.DMA((pieces["q"],)),
            ],
            compiler_params=pltpu.CompilerParams(collective_id=0, has_side_effects=True, vmem_limit_bytes=VMEM),
        )(x, gain, wq, wk, wv, wo, freq)
        return y

    tokens, whole = P(("dp", "sp"), None), P("sp", None)
    return jax.shard_map(
        step,
        mesh=mesh,
        in_specs=(tokens, P(None), whole, whole, whole, whole),
        out_specs=tokens,
        check_vma=False,
    )
```

```python
import functools

import jax
import jax.numpy as jnp
import numpy as np
from jax import lax
from jax.experimental import pallas as pl
from jax.experimental.pallas import tpu as pltpu
from jax.sharding import PartitionSpec as P

HEAD = 128
THETA = 10000
NEG = -1e30
HIDDEN = 2 * NEG
LOG2E = 1.4426950408889634
VMEM = 58 * 2**20
MESH = pl.DeviceIdType.MESH
WIDTH = {"w": 256, "q": 512, "o": 256}
SHARED = {"w": 0, "q": 0, "o": 4}
PARTLY = 1
SLOTS = 4

PLAN = [
    ("own", "w0"), ("own", "o15"), ("own", "o13"), ("angles", ""), ("own", "q3"), ("own", "w1"), ("state", ""), ("near", "w0"),
    ("near", "q3"), ("near", "w1"), ("far", "w0"), ("load", "w0"), ("far", "q3"), ("own", "q0"), ("load", "q3"), ("far", "w1"),
    ("Q", "q3"), ("load", "w1"), ("W", "w0"), ("own", "kv"), ("near", "q0"), ("near", "kv"), ("far", "q0"), ("own", "q2"),
    ("load", "q0"), ("Q", "q0"), ("far", "kv"), ("own", "o0"), ("have", "kv"), ("A", "q3"), ("near", "q2"), ("own", "o1"),
    ("own", "o2"), ("A", "q0"), ("near", "o0"), ("take", ""), ("V", "w0"), ("far", "q2"), ("own", "pv"), ("R", "q3"),
    ("near", "o1"), ("load", "q2"), ("R", "q0"), ("near", "o2"), ("Q", "q2"), ("near", "o15"), ("R", "q2"), ("far", "o0"),
    ("A", "q2"), ("near", "o14"), ("near", "pv"), ("far", "o1"), ("own", "q1"), ("own", "o11"), ("far", "o2"), ("near", "o13"),
    ("far", "pv"), ("own", "o4"), ("far", "o15"), ("have", "pv"), ("B", "q3"), ("give", "q3"), ("near", "q1"), ("far", "o14"),
    ("own", "o8"), ("own", "o12"), ("own", "o14"), ("own", "o9"), ("B", "q0"), ("give", "q0"), ("near", "o4"), ("near", "o11"),
    ("far", "o13"), ("B", "q2"), ("give", "q2"), ("near", "o8"), ("far", "q1"), ("own", "o10"), ("own", "o3"), ("near", "o9"),
    ("load", "q1"), ("load", "o0"), ("load", "o1"), ("load", "o14"), ("load", "o15"), ("Q", "q1"), ("far", "o4"), ("R", "q1"),
    ("B", "q1"), ("give", "q1"), ("near", "o3"), ("near", "o10"), ("far", "o8"), ("own", "o5"), ("own", "o7"), ("own", "o6"),
    ("load", "o2"), ("A", "q1"), ("far", "o3"), ("far", "o9"), ("far", "o11"), ("load", "o8"), ("load", "o3"), ("load", "o9"),
    ("far", "o10"), ("seen", ""), ("O", "o0"), ("load", "o10"), ("load", "o11"), ("O", "o14"), ("near", "o5"), ("load", "o4"),
    ("O", "o2"), ("near", "o7"), ("O", "o8"), ("near", "o6"), ("near", "o12"), ("load", "o13"), ("O", "o10"), ("far", "o5"),
    ("load", "o5"), ("far", "o7"), ("far", "o12"), ("O", "o4"), ("far", "o6"), ("load", "o7"), ("load", "o12"), ("load", "o6"),
    ("O", "o12"), ("O", "o6"),
]


def _dot(a, b, ca, cb):
    return lax.dot_general(a, b, (((ca,), (cb,)), ((), ())), preferred_element_type=jnp.float32)


def _kernel(n, x_hbm, gain_ref, wq, wk, wv, wo, freq_ref, y_ref, got_w, got_q, got_o,
            x_s, left_s, out_s, k_s, v_s, w_s, q_s, acc_s, top_s, prev_s, mix_s, score_s, cos_s, sin_s,
            near_sem, core_sem, send_sem, load_sem, x_sem, state_sem, give_sem, seen_sem):
    tokens, width = x_s.shape
    got = {"w": got_w, "q": got_q, "o": got_o}
    pieces = {kind: got[kind].shape[0] for kind in got}
    base = {"w": 0, "q": pieces["w"], "o": pieces["w"] + pieces["q"]}
    at_k = sum(pieces.values())
    depth = wq.shape[0]
    per = WIDTH["q"] // HEAD
    group = width // HEAD // (wk.shape[1] // HEAD)

    me = lax.axis_index("sp")
    dp = lax.axis_index("dp")
    side = lax.rem(me, 2)
    odd = lax.rem(dp, 2)
    right, left, opp = lax.rem(me + 2, n), lax.rem(me + n - 2, n), lax.rem(me + n // 2, n)
    core = me + 1 - 2 * side
    from_near = (left, right, opp)
    from_core = (core, lax.rem(core + n - 2, n), lax.rem(core + 2, n), lax.rem(core + n // 2, n))
    to_right, to_left, to_core = {"sp": right}, {"sp": left}, {"sp": core}
    to_peer = {"dp": dp + 1 - 2 * odd}
    onward = lax.select(side == 0, right, left)
    carried = lax.select(side == 0, left, right)

    def piece(kind, j):
        return j + odd * (pieces[kind] - 1 - 2 * j) if kind == "o" else j

    def index(kind, j):
        return base[kind] + piece(kind, j)

    def along_x(kind, j):
        return j < pieces[kind] - SHARED[kind]

    def exported(kind, j):
        return j < SHARED[kind]

    def far_exported(kind, j):
        return kind == "o" and j < SHARED[kind] + PARTLY

    def relayed(kind, j):
        return kind != "o" or j < pieces[kind] - SHARED[kind] - PARTLY

    def own_block(kind, j, act):
        ref = {"w": (wk, wv)[j % 2], "q": wq, "o": wo}[kind]
        at = {"w": odd, "q": odd * pieces["q"] + j, "o": piece(kind, j)}[kind]
        act(ref.at[:, pl.ds(pl.multiple_of(at * WIDTH[kind], WIDTH[kind]), WIDTH[kind])])

    def send(src, dst, send_at, recv, to):
        pltpu.make_async_remote_copy(src_ref=src, dst_ref=dst, send_sem=send_sem.at[send_at], recv_sem=recv, device_id=to,
                                     device_id_type=MESH).start()

    def arrived(ref, sem):
        pltpu.make_async_copy(ref, ref, sem).wait()

    def parts(kind, j):
        if kind in ("kv", "pv"):
            seq = ("kv", "pv").index(kind)
            return [(at_k + 2 * seq, lambda s: k_s.at[seq, s]), (at_k + 2 * seq + 1, lambda s: v_s.at[seq, s])]
        p = piece(kind, j)
        return [(base[kind] + p, lambda s: got[kind].at[p, s])]

    def own(kind, j):
        def act(src, i, block):
            if kind in ("kv", "pv") or along_x(kind, j):
                send(src, block(me), i, near_sem.at[i, 0], to_right)
                send(src, block(me), i, near_sem.at[i, 1], to_left)
            send(src, block(me), i, core_sem.at[i, 0], to_core)

        for i, block in parts(kind, j):
            if kind in ("kv", "pv"):
                act(block(me), i, block)
            else:
                own_block(kind, j, lambda src: act(src, i, block))

    def near(kind, j):
        for i, block in parts(kind, j):
            for slot in (0, 1):
                s = from_near[slot]
                arrived(block(s), near_sem.at[i, slot])
                if kind == "o" and exported(kind, j):
                    send(block(s), block(s), i, near_sem.at[i, slot], to_peer)
            if relayed(kind, j):
                send(block(carried), block(carried), i, near_sem.at[i, 2], {"sp": onward})
            for slot in (0, 1):
                s = from_near[slot]
                send(block(s), block(s), i, core_sem.at[i, 1 + slot], to_core)

    def far(kind, j):
        for i, block in parts(kind, j):
            arrived(block(opp), near_sem.at[i, 2])
            if far_exported(kind, j):
                send(block(opp), block(opp), i, near_sem.at[i, 2], to_peer)
            send(block(opp), block(opp), i, core_sem.at[i, 3], to_core)

    def have(kind, j):
        for i, block in parts(kind, j):
            for slot in range(4):
                arrived(block(from_core[slot]), core_sem.at[i, slot])

    def load(kind, j, slot):
        have(kind, j)
        p = piece(kind, j)
        b = WIDTH[kind]
        half = pl.ds(pl.multiple_of(lax.rem(p, WIDTH["q"] // b) * b, b), b)
        own_block(kind, j, lambda src: pltpu.make_async_copy(src, w_s.at[slot, me, :, half], load_sem.at[slot]).start())
        for far_off in range(1, n):
            s = lax.rem(me + far_off, n)
            pltpu.make_async_copy(got[kind].at[p, s], w_s.at[slot, s, :, half], load_sem.at[slot]).start()

    def product(which, slot):
        acc_s[...] = jnp.dot(left_s[which], w_s[slot].reshape(n * depth, WIDTH["q"]), preferred_element_type=jnp.float32)

    def turned(h):
        t = acc_s[:, h * HEAD : (h + 1) * HEAD].astype(jnp.bfloat16).astype(jnp.float32)
        return (t * cos_s[...] + pltpu.roll(t, HEAD // 2, 1) * sin_s[...]).astype(jnp.bfloat16)

    parts_of_state = 4

    def quarter(r):
        size = tokens // parts_of_state
        return pl.ds(pl.multiple_of(r * size, size), size)

    def norm(first):
        step = 32

        def some(r, _):
            here = pl.ds(pl.multiple_of(first * (tokens // parts_of_state) + r * step, step), step)
            wide = x_s[here, :].astype(jnp.float32)
            scale = lax.rsqrt(jnp.mean(wide * wide, -1, keepdims=True) + 1e-6)
            left_s[0, here, :] = (wide * scale * gain_ref[...].astype(jnp.float32)[None]).astype(jnp.bfloat16)
        lax.fori_loop(0, tokens // parts_of_state // step, some, None)

    def states():
        arrived(x_s, x_sem)

        def some(r, _):
            norm(r)
            pltpu.make_async_remote_copy(src_ref=left_s.at[0, quarter(r)], dst_ref=left_s.at[2, quarter(r)], send_sem=state_sem.at[0, r],
                                         recv_sem=state_sem.at[1, r], device_id=to_peer, device_id_type=MESH).start()
        lax.fori_loop(0, parts_of_state, some, None)

    def angles():
        step = 128

        def some(r, _):
            here = pl.ds(pl.multiple_of(r * step, step), step)
            place = me * tokens + r * step + lax.broadcasted_iota(jnp.int32, (step, HEAD), 0)
            angle = place.astype(jnp.float32) * freq_ref[...]
            cos_s[here, :] = jnp.cos(angle)
            sin = jnp.sin(angle)
            sin_s[here, :] = jnp.where(lax.broadcasted_iota(jnp.int32, (step, HEAD), 1) < HEAD // 2, -sin, sin)
        lax.fori_loop(0, tokens // step, some, None)

    e = HEAD**-0.5 * LOG2E

    def attend(seq, p):
        kv_head = lax.div(p * per, group)
        for h in range(per):
            top_s[h : h + 1, :] = jnp.full((1, tokens), NEG, jnp.float32)
            mix_s[h] = jnp.zeros((HEAD + 8, tokens), jnp.float32)

        def score(b, h, masked):
            s = _dot(k_s[seq, b, kv_head], q_s[seq, p, h], 1, 1)
            if masked:
                shape = (tokens, tokens)
                s = jnp.where(lax.broadcasted_iota(jnp.int32, shape, 1) >= lax.broadcasted_iota(jnp.int32, shape, 0), s, HIDDEN)
            old = top_s[h : h + 1, :]
            prev_s[h : h + 1, :] = old
            top_s[h : h + 1, :] = jnp.maximum(old, s.max(axis=0, keepdims=True))
            score_s[h] = s

        def weigh(b, coming):
            values = jnp.concatenate([v_s[seq, b, kv_head], jnp.ones((8, tokens), jnp.bfloat16)], axis=0)
            for h in range(per):
                top = top_s[h : h + 1, :]
                weights = jnp.exp2((score_s[h] - top) * e).astype(jnp.bfloat16)
                keep = jnp.exp2((prev_s[h : h + 1, :] - top) * e)
                if coming is not None:
                    score(coming, h, False)
                mix_s[h] = mix_s[h] * keep + _dot(values, weights, 1, 0)

        for h in range(per):
            score(me, h, True)
        lax.fori_loop(0, me, lambda b, _: weigh(lax.select(b == 0, me, b - 1), b), None)
        weigh(lax.select(me == 0, me, me - 1), None)
        for h in range(per):
            out = mix_s[h, :HEAD, :] * (1 / mix_s[h, HEAD : HEAD + 1, :])
            out = out.T.astype(jnp.bfloat16)

            @pl.when(seq == 0)
            def _():
                left_s[1, :, pl.ds(pl.multiple_of(((odd * pieces["q"] + p) * per + h) * HEAD, HEAD), HEAD)] = out

            @pl.when(seq == 1)
            def _():
                out_s[p, :, h * HEAD : (h + 1) * HEAD] = out

    def mine(p):
        b = WIDTH["q"]
        return pl.ds(pl.multiple_of((odd * pieces["q"] + p) * b, b), b)

    def give(p):
        pltpu.make_async_remote_copy(src_ref=out_s.at[p], dst_ref=left_s.at[1, :, mine(p)], send_sem=give_sem.at[p], recv_sem=seen_sem.at[p],
                                     device_id=to_peer, device_id_type=MESH).start()

    def seen():
        for p in range(pieces["q"]):
            arrived(out_s.at[p], seen_sem.at[p])

    def project(p):
        b = WIDTH["q"]
        at = pl.ds(pl.multiple_of(lax.div(p, 2) * b, b), b)
        y_ref[:, at] = (x_s[:, at].astype(jnp.float32) + acc_s[...]).astype(jnp.bfloat16)

    def keys(seq):
        heads = WIDTH["w"] // HEAD
        for h in range(heads):
            k_s[seq, me, h] = turned(h)
            v_s[seq, me, h] = acc_s[:, (heads + h) * HEAD : (heads + h + 1) * HEAD].astype(jnp.bfloat16).T

    def queries(seq, p):
        for h in range(per):
            q_s[seq, p, h] = turned(h)

    pltpu.make_async_copy(x_hbm, x_s, x_sem).start()
    barrier = pltpu.get_barrier_semaphore()
    partners = [to_right, to_left, to_core, to_peer]

    for to in partners:
        pl.semaphore_signal(barrier, inc=1, device_id=to, device_id_type=MESH)

    names = "WVQRABO"
    steps, events, slots, place = [], [], [], {}
    for what, token in PLAN:
        kind, j = (token, 0) if not token[-1:].isdigit() else (token[0], int(token[1:]))
        key = (kind, j if kind == "q" else j // 2)
        if what in names:
            steps.append((what, kind, j, events))
            slots.append(place.get(key, 0))
            events = []
        else:
            if what == "load" and key not in place:
                place[key] = len(place) % SLOTS
            events.append((what, kind, j, place.get(key, 0)))
    tail = events
    acts = {"own": own, "near": near, "far": far, "have": have}

    def run(events):
        for what, kind, j, slot in events:
            with jax.named_scope(f"{what}_{kind}_{j}"):
                if what == "angles":
                    angles()
                elif what == "state":
                    states()
                elif what == "take":
                    for r in range(parts_of_state):
                        arrived(left_s.at[2, quarter(r)], state_sem.at[1, r])
                elif what == "give":
                    give(j)
                elif what == "seen":
                    seen()
                elif what == "load":
                    load(kind, j, slot)
                else:
                    acts[what](kind, j)

    def pick(step, values, first=0):
        if len(set(values)) == 1:
            return jnp.int32(values[0])
        half = len(values) // 2
        return jnp.where(step < first + half, pick(step, values[:half], first), pick(step, values[half:], first + half))

    def choose(step, first, end):
        if not any(steps[m][3] for m in range(first, end)):
            return
        if end - first == 1:
            run(steps[first][3])
            return
        half = (first + end) // 2
        pl.when(step < half)(lambda: choose(step, first, half))
        pl.when(step >= half)(lambda: choose(step, half, end))

    def go(step, _):
        choose(step, 0, len(steps))
        code = pick(step, [names.index(what) + 8 * (slot + 8 * j) for (what, _, j, _), slot in zip(steps, slots)])
        what, slot, j = code & 7, (code >> 3) & 7, code >> 6
        seq = what & 1
        p = jnp.where(what == 6, j + odd * (pieces["o"] - 1 - 2 * j), j)
        state = 2 * seq

        @pl.when((what < 4) | (what == 6))
        def _():
            with jax.named_scope("wait"):
                pl.when((what & 1) == 0)(lambda: arrived(w_s.at[slot], load_sem.at[slot]))
            with jax.named_scope("product"):
                product(jnp.where(what == 6, 1, state), slot)
                pl.when(what < 2)(lambda: keys(seq))
                pl.when((what == 2) | (what == 3))(lambda: queries(seq, p))
                pl.when(what == 6)(lambda: project(p))

        @pl.when((what == 4) | (what == 5))
        def _():
            with jax.named_scope("attend"):
                attend(seq, p)

    with jax.named_scope("barrier"):
        pl.semaphore_wait(barrier, len(partners))

    lax.fori_loop(0, len(steps), go, None)
    run(tail)

    for kind in ("w", "q", "o"):
        for j in range(pieces[kind]):
            count = 4 + 2 * along_x(kind, j) + relayed(kind, j) + 2 * exported(kind, j) + far_exported(kind, j)
            half = 2 - count % 2
            sent = got[kind].at[pl.ds(0, half), pl.ds(0, count // half)]
            arrived(sent, send_sem.at[index(kind, j)])
    for seq in range(2):
        arrived(k_s.at[seq, pl.ds(0, 7)], send_sem.at[at_k + 2 * seq])
        arrived(v_s.at[seq, pl.ds(0, 7)], send_sem.at[at_k + 2 * seq + 1])
    for r in range(parts_of_state):
        arrived(left_s.at[0, quarter(r)], state_sem.at[0, r])
    for p in range(pieces["q"]):
        arrived(out_s.at[p], give_sem.at[p])


def solution(mesh):
    n = mesh.shape["sp"]

    def step(x, gain, wq, wk, wv, wo):
        tokens, width = x.shape
        half = HEAD // 2
        freq = np.float32(THETA) ** (-np.arange(half, dtype=np.float32) / np.float32(half))
        freq = jnp.asarray(np.concatenate([freq, freq])[None])
        pieces = {"w": wk.shape[1] // WIDTH["w"], "q": wq.shape[1] // WIDTH["q"] // 2, "o": wo.shape[1] // WIDTH["o"]}
        got = {kind: (pieces[kind], n, wq.shape[0], WIDTH[kind]) for kind in pieces}
        chunks = sum(pieces.values())
        per = WIDTH["q"] // HEAD
        heads = wk.shape[1] // HEAD // 2
        bf = jnp.bfloat16
        anywhere, vmem = pl.BlockSpec(memory_space=pl.ANY), pl.BlockSpec(memory_space=pltpu.VMEM)
        y, *_ = pl.pallas_call(
            functools.partial(_kernel, n),
            out_shape=[pltpu.VMEM(x.shape, bf), *(jax.ShapeDtypeStruct(got[kind], bf) for kind in "wqo")],
            in_specs=[anywhere, vmem, anywhere, anywhere, anywhere, anywhere, vmem],
            out_specs=[vmem, anywhere, anywhere, anywhere],
            scratch_shapes=[
                pltpu.VMEM((tokens, width), bf),
                pltpu.VMEM((3, tokens, width), bf),
                pltpu.VMEM((pieces["q"], tokens, WIDTH["q"]), bf),
                pltpu.VMEM((2, n, heads, tokens, HEAD), bf),
                pltpu.VMEM((2, n, heads, HEAD, tokens), bf),
                pltpu.VMEM((SLOTS, *got["q"][1:]), bf),
                pltpu.VMEM((2, pieces["q"], per, tokens, HEAD), bf),
                pltpu.VMEM((tokens, WIDTH["q"]), jnp.float32),
                pltpu.VMEM((per, tokens), jnp.float32),
                pltpu.VMEM((per, tokens), jnp.float32),
                pltpu.VMEM((per, HEAD + 8, tokens), jnp.float32),
                pltpu.VMEM((per, tokens, tokens), jnp.float32),
                pltpu.VMEM((tokens, HEAD), jnp.float32),
                pltpu.VMEM((tokens, HEAD), jnp.float32),
                pltpu.SemaphoreType.DMA((chunks + 4, 3)),
                pltpu.SemaphoreType.DMA((chunks + 4, 4)),
                pltpu.SemaphoreType.DMA((chunks + 4,)),
                pltpu.SemaphoreType.DMA((SLOTS,)),
                pltpu.SemaphoreType.DMA,
                pltpu.SemaphoreType.DMA((2, 4)),
                pltpu.SemaphoreType.DMA((pieces["q"],)),
                pltpu.SemaphoreType.DMA((pieces["q"],)),
            ],
            compiler_params=pltpu.CompilerParams(collective_id=0, has_side_effects=True, vmem_limit_bytes=VMEM),
        )(x, gain, wq, wk, wv, wo, freq)
        return y

    tokens, whole = P(("dp", "sp"), None), P("sp", None)
    return jax.shard_map(
        step,
        mesh=mesh,
        in_specs=(tokens, P(None), whole, whole, whole, whole),
        out_specs=tokens,
        check_vma=False,
    )
```
